32 devices in a mesh: mp: 4 (over y, x), nodes: 8 (over z, core).
Axes of the slice: x: 2, y: 2, z: 4, core: 2. Of those that a mesh axis runs over, the one named last changes fastest.
Arguments:
- grid_latent: float32 [16384, 512], P('nodes'), may hold values from -6 to 6
- mesh_latent: float32 [1024, 512], P('nodes'), may hold values from -250 to 250
- enc_grid_w: float32 [512, 512], P(None, 'mp'), may hold values from -0.25 to 0.25
- enc_mesh_w: float32 [512, 512], P(None, 'mp'), may hold values from -0.25 to 0.25
- enc_out_w: float32 [512, 512], P('mp'), may hold values from -0.25 to 0.25
- block_gain: float32 [512], replicated, may hold values from 0.5 to 1.5
- query_w: float32 [512, 512], P(None, 'mp'), may hold values from -1 to 1
- key_w: float32 [512, 512], P(None, 'mp'), may hold values from -1 to 1
- value_w: float32 [512, 512], P(None, 'mp'), may hold values from -0.25 to 0.25
- out_w: float32 [512, 512], P('mp'), may hold values from -0.25 to 0.25
- up_w: float32 [512, 2048], P(None, 'mp'), may hold values from -0.25 to 0.25
- down_w: float32 [2048, 512], P('mp'), may hold values from -0.125 to 0.125
- dec_gain: float32 [512], replicated, may hold values from 0.5 to 1.5
- dec_grid_w: float32 [512, 512], P(None, 'mp'), may hold values from -0.25 to 0.25
- dec_mesh_w: float32 [512, 512], P(None, 'mp'), may hold values from -0.25 to 0.25
- dec_out_w: float32 [512, 512], P('mp'), may hold values from -0.25 to 0.25
- neighbor_blocks: int32 [8, 16], replicated, may hold values from 0 to 7, as said below
- enc_tiles: int32 [256, 2], P('nodes'), may hold values from -1 to 127, as said below
- enc_edges: int32 [256, 2, 128], P('nodes'), may hold values from 0 to 127
- dec_tiles: int32 [384, 2], P('nodes'), may hold values from 0 to 127, as said below
- dec_edges: int32 [384, 2, 128], P('nodes'), may hold values from 0 to 127
Outputs:
- grid_out: float32 [16384, 512], P('nodes', 'mp')
The draws below stay inside these ranges and needn't reach their ends.
Inputs may be any that keep to these rules, and one draw needn't show every extreme that they name: `neighbor_blocks`: rows i * 1 to (i + 1) - 1 are the query blocks of index i of nodes; among all entries of those rows, the blocks of any one index j of nodes (ids j * 1 to (j + 1) - 1) are named at most 4 times, and for every i some j is named exactly 4 times. Entries may repeat. `enc_tiles`: tile slots i * 32 to (i + 1) * 32 - 1 belong to index i of nodes; a live tile names a grid block and a mesh block both of index i; an unused slot holds -1 in both columns; on each index the live slots come first, their number differs between indices, and some index has all 32 slots live. `dec_tiles`: tiles i * 48 to (i + 1) * 48 - 1 belong to index i of nodes; each names a grid block of index i and a mesh block of index i - 1, i or i + 1 of nodes (counted around the axis).
All inputs are finite; a program needn't handle non-finite values.
Results may differ from the reference program's by a relative error of at most 0.000098.
Values sent between devices are 32-bit elements; how exact they have to be, the bound alone decides.
No kernel may reach another device: no remote copies, remote signals or barrier semaphores. Data moves between devices by JAX's collectives and lax.ppermute only.
A program may use at most 128 MiB of HBM per device.

```python
import math
import jax
import jax.numpy as jnp
from jax import lax

D = 512
HEADS = 4
HEAD_DIM = 128
FF = 2048
EDGE_HIDDEN = 512
NODE_BLOCK = 128
NBR = 16
GRID_DEV = 2048
BPD = 1
GRID = 16384
MBLOCKS = 8
MESH = 1024
ET_DEV = 32
DT_DEV = 48
ETILES = 256
DTILES = 384


def drawn_weight(key, salt):
    entries = jax.random.normal(jax.random.fold_in(key, salt), (D, D), jnp.float32)
    return jnp.clip(entries, -4.0, 4.0) / math.sqrt(D)


def draw_query_w(key, part):
    weight_rows = drawn_weight(key, 61)
    return weight_rows


def draw_key_w(key, part):
    weight_rows = drawn_weight(key, 62)
    return weight_rows


def draw_mesh_latent(key, part):
    latent = jnp.clip(jax.random.normal(jax.random.fold_in(key, 71), (MESH, D), jnp.float32), -6.0, 6.0)
    return latent


def draw_neighbor_blocks(key, part):
    devices = MBLOCKS // BPD
    request_count = BPD * NBR
    slot_count = max(1, 2 * request_count // devices)

    def one_device(device_key):
        first, second, third = jax.random.split(device_key, 3)
        order = jax.random.permutation(first, devices)
        owners = order[jnp.arange(request_count) // slot_count]
        within_owner = jax.random.randint(second, (request_count,), 0, BPD)
        mixing = jax.random.permutation(third, request_count)
        return (owners * BPD + within_owner)[mixing]
    device_keys = jax.random.split(jax.random.fold_in(key, 11), devices)
    listed = jax.vmap(one_device)(device_keys)
    return listed.reshape(MBLOCKS, NBR).astype(jnp.int32)


def draw_enc_tiles(key, part):
    devices = MBLOCKS // BPD
    per_device = ET_DEV
    grid_blocks = GRID_DEV // NODE_BLOCK
    first, second, third, fourth = jax.random.split(jax.random.fold_in(key, 23), 4)
    raw_count = jax.random.randint(first, (devices,), 0, per_device)
    used = 1 + raw_count * raw_count // per_device
    busiest = jax.random.randint(second, (), 0, devices)
    used = jnp.where(jnp.arange(devices) == busiest, per_device, used)
    tile_live = jnp.arange(per_device)[None, :] < used[:, None]
    device = jnp.arange(devices)[:, None]
    source = device * grid_blocks + jax.random.randint(third, (devices, per_device), 0, grid_blocks)
    target = device * BPD + jax.random.randint(fourth, (devices, per_device), 0, BPD)
    tile_ids = jnp.stack([jnp.where(tile_live, source, -1), jnp.where(tile_live, target, -1)], axis=-1)
    return tile_ids.reshape(devices * per_device, 2).astype(jnp.int32)


def draw_dec_tiles(key, part):
    devices = MBLOCKS // BPD
    per_device = DT_DEV
    grid_blocks = GRID_DEV // NODE_BLOCK
    first, second, third = jax.random.split(jax.random.fold_in(key, 37), 3)
    device = jnp.arange(devices)[:, None]
    beside = jax.random.randint(first, (devices, per_device), -1, 2)
    source = (device + beside) % devices * BPD + jax.random.randint(second, (devices, per_device), 0, BPD)
    target = device * grid_blocks + jax.random.randint(third, (devices, per_device), 0, grid_blocks)
    tile_ids = jnp.stack([source, target], axis=-1)
    return tile_ids.reshape(devices * per_device, 2).astype(jnp.int32)


def with_ends(values, stream_key, least, high):
    shape = values.shape
    index_at = [jax.random.randint(jax.random.fold_in(stream_key, axis), (), 0, shape[axis]) for axis in range(len(shape))]
    values = values.at[tuple(index_at)].set(least)
    longest = shape.index(max(shape))
    index_at[longest] = (index_at[longest] + 1) % shape[longest]
    return values.at[tuple(index_at)].set(high)


def block_scale(own_key, dims, pieces, low, largest):
    factor_of = 1.0
    for position, blocks in pieces:
        steps = jax.random.uniform(jax.random.fold_in(jax.random.fold_in(own_key, 6), position), (blocks,), jnp.float32, low / len(pieces), largest / len(pieces))
        factor_of = factor_of * jnp.repeat(jnp.exp(steps), dims[position] // blocks).reshape((-1,) + (1,) * (len(dims) - 1 - position))
    return factor_of


def centred(stream_key, dims, scale, most, shards=(), dtype=jnp.bfloat16):
    level = block_scale(stream_key, dims, shards, -0.22, 0.18) if shards else 1.0
    values = jax.random.normal(stream_key, dims, jnp.float32) * scale * level
    return jnp.minimum(jnp.maximum(values, -most), most).astype(dtype)


def setup_inputs(seed: int = 0) -> dict:
    arg_keys = jax.random.split(jax.random.key(seed), 22)
    return {
        "grid_latent": centred(arg_keys[0], (GRID, D), 1.0, 6.0, ((0, 8),), jnp.float32),
        "mesh_latent": draw_mesh_latent(jax.random.fold_in(arg_keys[21], 71), 0),
        "enc_grid_w": centred(arg_keys[2], (D, EDGE_HIDDEN), D ** -0.5, 0.25, ((1, 4),), jnp.float32),
        "enc_mesh_w": centred(arg_keys[3], (D, EDGE_HIDDEN), D ** -0.5, 0.25, ((1, 4),), jnp.float32),
        "enc_out_w": centred(arg_keys[4], (EDGE_HIDDEN, D), EDGE_HIDDEN ** -0.5, 0.25, ((0, 4),), jnp.float32),
        "block_gain": jnp.clip(1.0 + 0.1 * jax.random.normal(arg_keys[5], (D,), jnp.float32), 0.5, 1.5),
        "query_w": draw_query_w(jax.random.fold_in(arg_keys[21], 71), 0),
        "key_w": draw_key_w(jax.random.fold_in(arg_keys[21], 71), 0),
        "value_w": centred(arg_keys[8], (D, D), D ** -0.5, 0.25, ((1, 4),), jnp.float32),
        "out_w": centred(arg_keys[9], (D, D), D ** -0.5, 0.25, ((0, 4),), jnp.float32),
        "up_w": centred(arg_keys[10], (D, FF), D ** -0.5, 0.25, ((1, 4),), jnp.float32),
        "down_w": centred(arg_keys[11], (FF, D), FF ** -0.5, 0.125, ((0, 4),), jnp.float32),
        "dec_gain": jnp.clip(1.0 + 0.1 * jax.random.normal(arg_keys[12], (D,), jnp.float32), 0.5, 1.5),
        "dec_grid_w": centred(arg_keys[13], (D, EDGE_HIDDEN), D ** -0.5, 0.25, ((1, 4),), jnp.float32),
        "dec_mesh_w": centred(arg_keys[14], (D, EDGE_HIDDEN), D ** -0.5, 0.25, ((1, 4),), jnp.float32),
        "dec_out_w": centred(arg_keys[15], (EDGE_HIDDEN, D), EDGE_HIDDEN ** -0.5, 0.25, ((0, 4),), jnp.float32),
        "neighbor_blocks": draw_neighbor_blocks(jax.random.fold_in(arg_keys[21], 71), 0),
        "enc_tiles": draw_enc_tiles(jax.random.fold_in(arg_keys[21], 71), 0),
        "enc_edges": with_ends(jax.random.randint(arg_keys[18], (ETILES, 2, NODE_BLOCK), 0, NODE_BLOCK), jax.random.fold_in(arg_keys[18], 1), 0, NODE_BLOCK - 1).astype(jnp.int32),
        "dec_tiles": draw_dec_tiles(jax.random.fold_in(arg_keys[21], 71), 0),
        "dec_edges": with_ends(jax.random.randint(arg_keys[20], (DTILES, 2, NODE_BLOCK), 0, NODE_BLOCK), jax.random.fold_in(arg_keys[20], 1), 0, NODE_BLOCK - 1).astype(jnp.int32),
    }


FULL_PRECISION = lax.Precision.HIGHEST

def product(matrix, weight):
    return jnp.dot(matrix, weight, precision=FULL_PRECISION, preferred_element_type=jnp.float32)

def layer_norm(inputs, scales):
    centre = lax.optimization_barrier(jnp.mean(inputs, axis=-1, keepdims=True))
    shifted = inputs - centre
    spread = lax.optimization_barrier(jnp.mean(shifted * shifted, axis=-1, keepdims=True))
    return shifted * lax.rsqrt(spread + 1e-05) * scales

def edge_pass(source_side, target_side, tile_ids, edge_ids, targets):
    tile_live = tile_ids[:, 0] >= 0
    source = jnp.where(tile_live, tile_ids[:, 0], 0)[:, None] * NODE_BLOCK + edge_ids[:, 0, :]
    target = jnp.where(tile_live, tile_ids[:, 1], 0)[:, None] * NODE_BLOCK + edge_ids[:, 1, :]
    message = jax.nn.silu(source_side[source] + target_side[target])
    message = message * tile_live[:, None, None].astype(jnp.float32)
    hidden_cols = message.shape[-1]
    return jax.ops.segment_sum(message.reshape(-1, hidden_cols), target.reshape(-1), num_segments=targets)

def attention(queries, key_rows, value_rows, neighbor_blocks):
    blocks = queries.shape[0] // NODE_BLOCK
    query_blocks = queries.reshape(blocks, NODE_BLOCK, HEADS, HEAD_DIM)
    key_blocks = key_rows.reshape(blocks, NODE_BLOCK, HEADS, HEAD_DIM)
    value_blocks = value_rows.reshape(blocks, NODE_BLOCK, HEADS, HEAD_DIM)

    def one_block(inputs):
        block_queries, listed = inputs
        near_keys = key_blocks[listed].reshape(-1, HEADS, HEAD_DIM)
        near_values = value_blocks[listed].reshape(-1, HEADS, HEAD_DIM)
        scores = jnp.einsum('qhd,khd->hqk', block_queries, near_keys, precision=FULL_PRECISION) / math.sqrt(HEAD_DIM)
        weights = jax.nn.softmax(scores, axis=-1)
        return jnp.einsum('hqk,khd->qhd', weights, near_values, precision=FULL_PRECISION)
    attended = lax.map(one_block, (query_blocks, neighbor_blocks))
    return attended.reshape(-1, HEADS * HEAD_DIM)

def reference(grid_latent, mesh_latent, enc_grid_w, enc_mesh_w, enc_out_w, block_gain, query_w, key_w, value_w, out_w, up_w, down_w, dec_gain, dec_grid_w, dec_mesh_w, dec_out_w, neighbor_blocks, enc_tiles, enc_edges, dec_tiles, dec_edges):
    grid_enc = product(grid_latent, enc_grid_w)
    mesh_enc = product(mesh_latent, enc_mesh_w)
    enc_agg = edge_pass(grid_enc, mesh_enc, enc_tiles, enc_edges, mesh_latent.shape[0])
    mesh_one = mesh_latent + product(enc_agg, enc_out_w)
    normed = layer_norm(mesh_one, block_gain)
    queries = product(normed, query_w)
    key_rows = product(normed, key_w)
    value_rows = product(normed, value_w)
    attended = attention(queries, key_rows, value_rows, neighbor_blocks)
    hidden = jax.nn.silu(product(normed, up_w))
    mesh_two = mesh_one + product(attended, out_w) + product(hidden, down_w)
    mesh_dec = product(layer_norm(mesh_two, dec_gain), dec_mesh_w)
    grid_dec = product(grid_latent, dec_grid_w)
    dec_agg = edge_pass(mesh_dec, grid_dec, dec_tiles, dec_edges, grid_latent.shape[0])
    return grid_latent + product(dec_agg, dec_out_w)
```

```python
import functools
import math

import jax
import jax.numpy as jnp
from jax import lax
from jax.experimental import pallas as pl
from jax.experimental.pallas import tpu as pltpu
from jax.sharding import PartitionSpec as P

HEAD_DIM = 128
NODE_BLOCK = 128
F32 = jnp.float32
BF16 = jnp.bfloat16
EXACT = lax.Precision.HIGHEST


def partner(index, step, count, back=False):
    if count & (count - 1) == 0:
        return index ^ step
    return (index - step) % count if back else (index + step) % count


def exchange(value, axis, step):
    count = lax.axis_size(axis)
    return lax.ppermute(value, axis, [(i, partner(i, step, count)) for i in range(count)])


def shifted(value, axis, step):
    count = lax.axis_size(axis)
    return lax.ppermute(value, axis, [(i, (i + step) % count) for i in range(count)])


def parts(value):
    high = value.astype(BF16)
    return high, (value - high.astype(F32)).astype(BF16)


def mm(left, right):
    return jnp.dot(left, right, preferred_element_type=F32)


def mm_nt(left, right):
    return lax.dot_general(left, right, (((1,), (1,)), ((), ())), preferred_element_type=F32)


def dot3(left, right):
    left_high, left_low = left if isinstance(left, tuple) else parts(left)
    right_high, right_low = right if isinstance(right, tuple) else parts(right)
    return mm(left_high, right_high) + (mm(left_high, right_low) + mm(left_low, right_high))


def dot_exact(left, right):
    return jnp.dot(left, right, precision=EXACT, preferred_element_type=F32)


def silu(value):
    half = 0.5 * value
    return half + half * jnp.tanh(half)


def layer_norm(value, gain):
    centre = jnp.mean(value, axis=-1, keepdims=True)
    moved = value - centre
    spread = jnp.mean(moved * moved, axis=-1, keepdims=True)
    return moved * lax.rsqrt(spread + 1e-05) * gain


def one_hot(ids):
    rows = lax.broadcasted_iota(jnp.int32, (NODE_BLOCK, NODE_BLOCK), 0)
    return jnp.where(rows == ids, 1.0, 0.0).astype(BF16)


def side_by_side(value):
    high, low = parts(value)
    return jnp.concatenate([high, low], axis=1)


def add_messages(sources, targets, ids, sum_ref, at):
    from_hot = one_hot(ids[0:1])
    to_hot = one_hot(ids[1:2])
    hots = jnp.concatenate([from_hot, from_hot, to_hot, to_hot], axis=0)
    before = mm(jnp.concatenate([sources, targets], axis=1), hots)
    message = side_by_side(silu(before))
    sum_ref[at] += mm_nt(message, jnp.concatenate([to_hot, to_hot], axis=1))


def call(kernel, out_shape, micros, **options):
    return pl.pallas_call(
        kernel,
        out_shape=out_shape,
        cost_estimate=pl.CostEstimate(
            flops=int(micros * 4e8), bytes_accessed=1 << 20, transcendentals=0
        ),
        **options,
    )


def vmem(count):
    return [pl.BlockSpec(memory_space=pltpu.VMEM)] * count


def smem(count):
    return [pl.BlockSpec(memory_space=pltpu.SMEM)] * count


def shape(*dims, dtype=F32):
    return jax.ShapeDtypeStruct(dims, dtype)


def limit(mib):
    return pltpu.CompilerParams(vmem_limit_bytes=mib << 20)


def encoder_kernel(
    grid_blocks,
    node_blocks,
    tiles,
    grid_latent,
    grid_w,
    mesh_latent,
    mesh_w,
    edges,
    out,
    grid_side,
    mesh_side,
    sums,
    w_high,
    w_low,
):
    step = pl.program_id(0)
    chunk = grid_latent.shape[0] // NODE_BLOCK

    @pl.when(step == 0)
    def _():
        w_high[...], w_low[...] = parts(grid_w[...])
        mesh_enc = dot3(mesh_latent[...], mesh_w[...])
        for b in range(node_blocks):
            block = mesh_enc[b * NODE_BLOCK : (b + 1) * NODE_BLOCK]
            mesh_side[b] = side_by_side(block.T)
        sums[...] = jnp.zeros_like(sums)

    grid_enc = dot3(grid_latent[...], (w_high[...], w_low[...]))
    for b in range(chunk):
        block = grid_enc[b * NODE_BLOCK : (b + 1) * NODE_BLOCK]
        grid_side[step * chunk + b] = side_by_side(block.T)

    @pl.when(step == pl.num_programs(0) - 1)
    def _():
        me = lax.axis_index("nodes")

        def one_tile(t, carry):
            @pl.when(tiles[t, 0] >= 0)
            def _():
                source = tiles[t, 0] - me * grid_blocks
                target = tiles[t, 1] - me * node_blocks
                add_messages(grid_side[source], mesh_side[target], edges[t], sums, target)

            return carry

        lax.fori_loop(0, edges.shape[0], one_tile, 0)
        for b in range(node_blocks):
            out[b * NODE_BLOCK : (b + 1) * NODE_BLOCK, :] = sums[b].T


def columns(own, got, other, step, rows):
    if step == 0:
        return own[...]
    mine = got[step - 1][rows, :]
    theirs = other[step - 1, rows, :]
    first = lax.axis_index("nodes") % 2 == 0
    return jnp.concatenate(
        [jnp.where(first, mine, theirs), jnp.where(first, theirs, mine)], axis=0
    )


def middle_kernel(count, *refs):
    mesh_latent, gain, query_w, key_w, value_w, own_w, other_w = refs[:7]
    sums = refs[7 : 7 + count]
    got_w = refs[7 + count : 6 + 2 * count]
    mesh_one_ref, normed_ref, query_ref, key_value_ref = refs[6 + 2 * count :]
    width = mesh_latent.shape[1]
    half = slice(0, other_w.shape[1])
    added = [0.0] * (width // NODE_BLOCK)
    for step in range(count):
        left = parts(sums[step][...])
        weight = columns(own_w, got_w, other_w, step, half)
        for j in range(width // NODE_BLOCK):
            rows = slice(j * sums[step].shape[1], (j + 1) * sums[step].shape[1])
            added[j] = added[j] + dot3(left, weight[rows])
    mesh_one = mesh_latent[...] + jnp.concatenate(added, axis=1)
    normed = layer_norm(mesh_one, gain[...])
    mesh_one_ref[...] = mesh_one
    normed_ref[...] = normed
    query_ref[...] = dot_exact(normed, query_w[...])
    cols = key_w.shape[1]
    key_value_ref[:, :cols] = dot_exact(normed, key_w[...])
    key_value_ref[:, cols:] = dot3(normed, value_w[...])


def hidden_kernel(count, normed, up_w, down_w, out, scratch):
    hidden = silu(dot3(normed[...], up_w[...]))
    scratch[...] = dot3(hidden, down_w[...])
    rows = out.shape[1]
    me = lax.axis_index("mp")
    for step in range(count):
        out[step] = scratch[pl.ds(partner(me, step, count) * rows, rows), :]


def attention_kernel(count, heads, repeats, query, *refs):
    pieces, out, scores = refs[:count], refs[count], refs[count + 1]
    blocks = query.shape[0] // NODE_BLOCK
    cols = query.shape[1]
    for q in range(blocks):
        for h in range(heads):
            lanes = slice(h * HEAD_DIM, (h + 1) * HEAD_DIM)
            own = query[q * NODE_BLOCK : (q + 1) * NODE_BLOCK, lanes] * (1.0 / math.sqrt(HEAD_DIM))
            top = jnp.full((NODE_BLOCK, 1), -1e30, F32)
            for i in range(count):
                for b in range(blocks):
                    keys = pieces[i][b * NODE_BLOCK : (b + 1) * NODE_BLOCK, lanes]
                    score = lax.dot_general(
                        own,
                        keys,
                        (((1,), (1,)), ((), ())),
                        precision=EXACT,
                        preferred_element_type=F32,
                    )
                    score = jnp.where(repeats[q, i * blocks + b] > 0, score, -1e30)
                    scores[i * blocks + b] = score
                    top = jnp.maximum(top, jnp.max(score, axis=-1, keepdims=True))
            total = jnp.zeros((NODE_BLOCK, 1), F32)
            result = jnp.zeros((NODE_BLOCK, HEAD_DIM), F32)
            value_lanes = slice(cols + h * HEAD_DIM, cols + (h + 1) * HEAD_DIM)
            for i in range(count):
                for b in range(blocks):
                    times = repeats[q, i * blocks + b].astype(F32)
                    weight = jnp.exp(scores[i * blocks + b] - top) * times
                    total = total + jnp.sum(weight, axis=-1, keepdims=True)
                    values = pieces[i][b * NODE_BLOCK : (b + 1) * NODE_BLOCK, value_lanes]
                    result = result + dot3(weight, values)
            out[q * NODE_BLOCK : (q + 1) * NODE_BLOCK, lanes] = result / total


def after_kernel(count, *refs):
    mesh_one, gain, own_out_w, own_mesh_w, other = refs[:5]
    attended = refs[5 : 5 + count]
    hidden = refs[5 + count : 5 + 2 * count]
    got = refs[5 + 2 * count : 4 + 3 * count]
    out, total = refs[4 + 3 * count :]
    width = mesh_one.shape[1]
    half = own_out_w.shape[0] // 2
    tall = own_mesh_w.shape[0] // 2
    me = lax.axis_index("mp")
    added = [0.0] * (width // NODE_BLOCK)
    for step in range(count):
        left = parts(attended[step][...])
        weight = columns(own_out_w, got, other, step, slice(0, half))
        for j in range(width // NODE_BLOCK):
            depth = attended[step].shape[1]
            added[j] = added[j] + dot3(left, weight[j * depth : (j + 1) * depth])
    total[...] = mesh_one[...] + jnp.concatenate(added, axis=1)
    rows = hidden[0].shape[0]
    for step in range(count):
        place = pl.ds(partner(me, step, count, back=True) * rows, rows)
        total[place, :] += hidden[step][...]
    normed = parts(layer_norm(total[...], gain[...]))
    for step in range(count):
        weight = columns(own_mesh_w, got, other, step, slice(half, half + tall))
        projected = dot3(normed, weight)
        cols = weight.shape[1]
        out[step * cols : (step + 1) * cols, :] = projected.T


def grid_kernel(count, skip, *refs):
    grid_latent, own_w, other = refs[:3]
    got = refs[3 : 2 + count]
    out, high, low = refs[2 + count :]
    cols = own_w.shape[1]
    tall = own_w.shape[0] // 2

    @pl.when(pl.program_id(0) == 0)
    def _():
        for step in range(count):
            lanes = slice(step * cols, (step + 1) * cols)
            weight = columns(own_w, got, other, step, slice(skip, skip + tall))
            high[:, lanes], low[:, lanes] = parts(weight)

    grid_dec = dot3(grid_latent[...], (high[...], low[...]))
    for b in range(grid_latent.shape[0] // NODE_BLOCK):
        out[b] = side_by_side(grid_dec[b * NODE_BLOCK : (b + 1) * NODE_BLOCK].T)


def decoder_kernel(count, node_blocks, all_blocks, *refs):
    tiles, edges, grid_side, own, before, behind, grid_latent = refs[:7]
    weights = refs[7 : 7 + count]
    out, mesh_side, sums = refs[7 + count :]
    grid_blocks = grid_side.shape[0]
    me = lax.axis_index("nodes")
    for i, side in enumerate((before, own, behind)):
        for b in range(node_blocks):
            block = side[:, b * NODE_BLOCK : (b + 1) * NODE_BLOCK]
            mesh_side[i * node_blocks + b] = side_by_side(block)
    sums[...] = jnp.zeros_like(sums)

    def one_tile(t, carry):
        source = lax.rem(tiles[t, 0] - (me - 1) * node_blocks + all_blocks, all_blocks)
        target = tiles[t, 1] - me * grid_blocks
        add_messages(mesh_side[source], grid_side[target], edges[t], sums, target)
        return carry

    lax.fori_loop(0, edges.shape[0], one_tile, 0)
    weight = jnp.concatenate([w[...] for w in weights], axis=0).T
    weight = parts(weight)

    def one_block(c, carry):
        result = dot3(weight, sums[c]).T
        place = pl.ds(pl.multiple_of(c * NODE_BLOCK, NODE_BLOCK), NODE_BLOCK)
        out[place, :] = grid_latent[place, :] + result
        return carry

    lax.fori_loop(0, grid_blocks, one_block, 0)


def stacked(weight):
    return jnp.concatenate(
        [weight[:, j : j + NODE_BLOCK] for j in range(0, weight.shape[1], NODE_BLOCK)], axis=0
    )


def per_device(
    grid_latent,
    mesh_latent,
    enc_grid_w,
    enc_mesh_w,
    enc_out_w,
    block_gain,
    query_w,
    key_w,
    value_w,
    out_w,
    up_w,
    down_w,
    dec_gain,
    dec_grid_w,
    dec_mesh_w,
    dec_out_w,
    neighbor_blocks,
    enc_tiles,
    enc_edges,
    dec_tiles,
    dec_edges,
):
    me_node = lax.axis_index("nodes")
    me_mp = lax.axis_index("mp")
    nodes = lax.axis_size("nodes")
    mp = lax.axis_size("mp")
    steps = range(1, mp)
    grid_rows, width = grid_latent.shape
    node_rows = mesh_latent.shape[0]
    grid_blocks = grid_rows // NODE_BLOCK
    node_blocks = node_rows // NODE_BLOCK
    hidden_cols = enc_grid_w.shape[1]
    head_cols = query_w.shape[1]
    heads = head_cols // HEAD_DIM
    parity = me_node % 2
    chunks = 4 if grid_blocks % 4 == 0 else 1
    chunk_rows = grid_rows // chunks

    def my_half(weight):
        rows = weight.shape[0] // 2
        return lax.dynamic_slice_in_dim(weight, parity * rows, rows, 0)

    enc_out = stacked(enc_out_w)
    enc_half = my_half(enc_out)
    enc_got = [exchange(enc_half, "mp", k) for k in steps]
    enc_other = exchange(jnp.stack(enc_got), "nodes", 1)

    enc_agg = call(
        functools.partial(encoder_kernel, grid_blocks, node_blocks),
        shape(node_rows, hidden_cols),
        8,
        grid_spec=pltpu.PrefetchScalarGridSpec(
            num_scalar_prefetch=1,
            grid=(chunks,),
            in_specs=[
                pl.BlockSpec((chunk_rows, width), lambda i, t: (i, 0)),
                *vmem(5 - 1),
            ],
            out_specs=pl.BlockSpec((node_rows, hidden_cols), lambda i, t: (0, 0)),
            scratch_shapes=[
                pltpu.VMEM((grid_blocks, hidden_cols, 2 * NODE_BLOCK), BF16),
                pltpu.VMEM((node_blocks, hidden_cols, 2 * NODE_BLOCK), BF16),
                pltpu.VMEM((node_blocks, hidden_cols, NODE_BLOCK), F32),
                pltpu.VMEM((width, hidden_cols), BF16),
                pltpu.VMEM((width, hidden_cols), BF16),
            ],
        ),
        compiler_params=limit(24),
    )(enc_tiles, grid_latent, enc_grid_w, mesh_latent, enc_mesh_w, enc_edges)
    aggs = [enc_agg] + [exchange(enc_agg, "mp", k) for k in steps]

    mesh_one, normed, queries, key_values = call(
        functools.partial(middle_kernel, mp),
        (
            shape(node_rows, width),
            shape(node_rows, width),
            shape(node_rows, head_cols),
            shape(node_rows, 2 * head_cols),
        ),
        3,
        in_specs=vmem(6 + 2 * mp),
        out_specs=vmem(4),
        compiler_params=limit(24),
    )(
        mesh_latent,
        block_gain.reshape(1, -1),
        query_w,
        key_w,
        value_w,
        enc_out,
        enc_other,
        *aggs,
        *enc_got,
    )

    order = []
    if nodes % 2 == 0:
        far = [key_values] + [shifted(key_values, "nodes", 2 * s) for s in range(1, nodes // 2)]
        near = exchange(jnp.stack(far), "nodes", 1)
        pieces = far + [near[s] for s in range(nodes // 2)]
        order = [(me_node - 2 * s) % nodes for s in range(nodes // 2)]
        order += [((me_node ^ 1) - 2 * s) % nodes for s in range(nodes // 2)]
    else:
        pieces = [key_values] + [shifted(key_values, "nodes", s) for s in range(1, nodes)]
        order = [(me_node - s) % nodes for s in range(nodes)]

    common = my_half_of_all = jnp.concatenate(
        [my_half(stacked(out_w)), my_half(dec_mesh_w), my_half(dec_grid_w)], axis=0
    )
    share = dec_out_w.shape[1] // mp

    def out_columns(index):
        return lax.dynamic_slice_in_dim(dec_out_w, index * share, share, 1)

    got = [
        exchange(
            jnp.concatenate([common, out_columns(partner(me_mp, k, mp))], axis=0), "mp", k
        )
        for k in steps
    ]
    other = exchange(jnp.stack([g[: common.shape[0]] for g in got]), "nodes", 1)
    dec_out = [out_columns(me_mp)] + [g[common.shape[0] :] for g in got]

    hidden_parts = call(
        functools.partial(hidden_kernel, mp),
        shape(mp, node_rows // mp, width),
        2,
        in_specs=vmem(3),
        out_specs=vmem(1)[0],
        scratch_shapes=[pltpu.VMEM((node_rows, width), F32)],
        compiler_params=limit(24),
    )(normed, up_w, down_w)
    hidden_sum = hidden_parts[0]
    for k in steps:
        hidden_sum = hidden_sum + exchange(hidden_parts[k], "mp", k)
    hidden = [hidden_sum] + [exchange(hidden_sum, "mp", k) for k in steps]

    own_lists = lax.dynamic_slice_in_dim(neighbor_blocks, me_node * node_blocks, node_blocks, 0)
    piece_blocks = jnp.stack(order)[:, None] * node_blocks + jnp.arange(node_blocks)[None, :]
    repeats = jnp.sum(
        (own_lists[:, :, None] == piece_blocks.reshape(1, 1, -1)).astype(jnp.int32), axis=1
    )
    attended = call(
        functools.partial(attention_kernel, nodes, heads),
        shape(node_rows, head_cols),
        3,
        in_specs=smem(1) + vmem(1 + nodes),
        out_specs=vmem(1)[0],
        scratch_shapes=[pltpu.VMEM((nodes * node_blocks, NODE_BLOCK, NODE_BLOCK), F32)],
        compiler_params=limit(24),
    )(repeats, queries, *pieces)
    attends = [attended] + [exchange(attended, "mp", k) for k in steps]

    dec_cols = dec_mesh_w.shape[1]
    mesh_dec = call(
        functools.partial(after_kernel, mp),
        shape(mp * dec_cols, node_rows),
        3,
        in_specs=vmem(4 + 3 * mp),
        out_specs=vmem(1)[0],
        scratch_shapes=[pltpu.VMEM((node_rows, width), F32)],
        compiler_params=limit(24),
    )(
        mesh_one,
        dec_gain.reshape(1, -1),
        stacked(out_w),
        dec_mesh_w,
        other,
        *attends,
        *hidden,
        *got,
    )

    skip = common.shape[0] - dec_grid_w.shape[0] // 2
    grid_side = call(
        functools.partial(grid_kernel, mp, skip),
        shape(grid_blocks, mp * dec_cols, 2 * NODE_BLOCK, dtype=BF16),
        6,
        grid=(chunks,),
        in_specs=[
            pl.BlockSpec((chunk_rows, width), lambda i: (i, 0)),
            *vmem(1 + mp),
        ],
        out_specs=pl.BlockSpec(
            (chunk_rows // NODE_BLOCK, mp * dec_cols, 2 * NODE_BLOCK), lambda i: (i, 0, 0)
        ),
        scratch_shapes=[pltpu.VMEM((width, mp * dec_cols), BF16)] * 2,
        compiler_params=limit(32),
    )(grid_latent, dec_grid_w, other, *got)

    before = shifted(mesh_dec, "nodes", 1)
    behind = shifted(mesh_dec, "nodes", -1)
    grid_share = lax.dynamic_slice_in_dim(grid_latent, me_mp * share, share, 1)
    return call(
        functools.partial(decoder_kernel, mp, node_blocks, node_blocks * nodes),
        shape(grid_rows, share),
        12,
        in_specs=smem(1) + vmem(6 + mp),
        out_specs=vmem(1)[0],
        scratch_shapes=[
            pltpu.VMEM((3 * node_blocks, mp * dec_cols, 2 * NODE_BLOCK), BF16),
            pltpu.VMEM((grid_blocks, mp * dec_cols, NODE_BLOCK), F32),
        ],
        compiler_params=limit(32),
    )(dec_tiles, dec_edges, grid_side, mesh_dec, before, behind, grid_share, *dec_out)


def solution(mesh):
    in_specs = (
        P("nodes", None),
        P("nodes", None),
        P(None, "mp"),
        P(None, "mp"),
        P("mp", None),
        P(),
        P(None, "mp"),
        P(None, "mp"),
        P(None, "mp"),
        P("mp", None),
        P(None, "mp"),
        P("mp", None),
        P(),
        P(None, "mp"),
        P(None, "mp"),
        P("mp", None),
        P(),
        P("nodes", None),
        P("nodes", None, None),
        P("nodes", None),
        P("nodes", None, None),
    )
    out_specs = P("nodes", "mp")
    return jax.shard_map(
        per_device, mesh=mesh, in_specs=in_specs, out_specs=out_specs, check_vma=False
    )
```

```python
import functools
import math

import jax
import jax.numpy as jnp
from jax import lax
from jax.experimental import pallas as pl
from jax.experimental.pallas import tpu as pltpu
from jax.sharding import PartitionSpec as P


HEAD_DIM = 128
NODE_BLOCK = 128
GROUP = 8
ENC_GROUP = 16
F32 = jnp.float32
BF16 = jnp.bfloat16
EXACT = lax.Precision.HIGHEST


def partner(index, step, count, back=False):
    if count & (count - 1) == 0:
        return index ^ step
    return (index - step) % count if back else (index + step) % count


def exchange(value, axis, step):
    count = lax.axis_size(axis)
    return lax.ppermute(value, axis, [(i, partner(i, step, count)) for i in range(count)])


def shifted(value, axis, step):
    count = lax.axis_size(axis)
    return lax.ppermute(value, axis, [(i, (i + step) % count) for i in range(count)])


def parts(value):
    high = value.astype(BF16)
    return high, (value - high.astype(F32)).astype(BF16)


def mm(left, right):
    return jnp.dot(left, right, preferred_element_type=F32)


def mm_nt(left, right):
    return lax.dot_general(left, right, (((1,), (1,)), ((), ())), preferred_element_type=F32)


def dot3(left, right):
    left_high, left_low = left if isinstance(left, tuple) else parts(left)
    right_high, right_low = right if isinstance(right, tuple) else parts(right)
    return mm(left_high, right_high) + (mm(left_high, right_low) + mm(left_low, right_high))


def dot_exact(left, right):
    return jnp.dot(left, right, precision=EXACT, preferred_element_type=F32)


def silu(value):
    half = 0.5 * value
    return half + half * jnp.tanh(half)


def layer_norm(value, gain):
    centre = jnp.mean(value, axis=-1, keepdims=True)
    moved = value - centre
    spread = jnp.mean(moved * moved, axis=-1, keepdims=True)
    return moved * lax.rsqrt(spread + 1e-05) * gain


def one_hot(ids):
    rows = lax.broadcasted_iota(jnp.int32, (NODE_BLOCK, NODE_BLOCK), 0)
    return jnp.where(rows == ids, 1.0, 0.0).astype(BF16)


def side_by_side(value):
    high, low = parts(value)
    return jnp.concatenate([high, low], axis=1)


def fill(listed, taken, group, spare):
    for i in range(group):
        listed[0, taken + i] = 0
        listed[1, taken + i] = 0
        listed[2, taken + i] = spare


def picked(side, ids):
    wide = jnp.broadcast_to(ids, side.shape)
    return jnp.take_along_axis(side, wide, axis=1, mode="promise_in_bounds")


def add_messages(listed, taken, edges, before, messages, sums):
    group = messages.shape[0]

    def one_group(n, carry):
        to_hots = []

        def gather(i):
            at = n * group + i
            ids = edges[listed[0, at]]
            to_hots.append(one_hot(ids[1:2]))
            target = jnp.minimum(listed[2, at], sums.shape[0] - 2)
            messages[i] = side_by_side(silu(before(listed[1, at], target, ids[0:1], ids[1:2])))

        def scatter(i):
            both = jnp.concatenate([to_hots[i], to_hots[i]], axis=1)
            sums[listed[2, n * group + i]] += mm_nt(messages[i], both)

        for i in range(group):
            gather(i)
            if i:
                scatter(i - 1)
        scatter(group - 1)
        return carry

    lax.fori_loop(0, (taken + group - 1) // group, one_group, 0)


def call(kernel, out_shape, micros, **options):
    return pl.pallas_call(
        kernel,
        out_shape=out_shape,
        cost_estimate=pl.CostEstimate(
            flops=int(micros * 4e8), bytes_accessed=1 << 20, transcendentals=0
        ),
        **options,
    )


def vmem(count):
    return [pl.BlockSpec(memory_space=pltpu.VMEM)] * count


def hbm(count):
    return [pl.BlockSpec(memory_space=pltpu.HBM)] * count


def smem(count):
    return [pl.BlockSpec(memory_space=pltpu.SMEM)] * count


def in_hbm(value):
    return pltpu.with_memory_space_constraint(value, pltpu.HBM)


def shape(*dims, dtype=F32):
    return jax.ShapeDtypeStruct(dims, dtype)


def limit(mib):
    return pltpu.CompilerParams(vmem_limit_bytes=mib << 20)


def row_chunks(source, target, sems, first=0):
    chunks = sems.shape[0] - first
    rows = source.shape[0] // chunks
    return [
        pltpu.make_async_copy(
            source.at[pl.ds(c * rows, rows)], target.at[pl.ds(c * rows, rows)], sems.at[first + c]
        )
        for c in range(chunks)
    ]


def encoder_kernel(
    grid_blocks,
    node_blocks,
    tiles,
    grid_latent,
    grid_w,
    mesh_latent,
    mesh_w,
    edges,
    out,
    grid_rows,
    grid_w_here,
    mesh_rows,
    mesh_w_here,
    edges_here,
    grid_side,
    mesh_side,
    sums,
    messages,
    listed,
    sems,
):
    small = [
        pltpu.make_async_copy(source, target, sems.at[i])
        for i, (source, target) in enumerate(
            [
                (grid_w, grid_w_here),
                (mesh_latent, mesh_rows),
                (mesh_w, mesh_w_here),
                (edges, edges_here),
            ]
        )
    ]
    large = row_chunks(grid_latent, grid_rows, sems, len(small))
    small[0].start()
    for copy in large:
        copy.start()
    for copy in small[1:]:
        copy.start()
    me = lax.axis_index("nodes")

    def sort_in(t, taken):
        listed[0, taken] = t
        listed[1, taken] = tiles[0, t] - me * grid_blocks
        listed[2, taken] = tiles[1, t] - me * node_blocks
        return taken + (tiles[0, t] >= 0).astype(jnp.int32)

    taken = lax.fori_loop(0, tiles.shape[1], sort_in, 0)
    fill(listed, taken, messages.shape[0], node_blocks)
    sums[...] = jnp.zeros_like(sums)
    small[0].wait()
    weight = parts(grid_w_here[...])
    rows = grid_rows.shape[0] // len(large)
    chunk = rows // NODE_BLOCK
    for c, copy in enumerate(large):
        copy.wait()
        grid_enc = dot3(grid_rows[c * rows : (c + 1) * rows], weight)
        for b in range(chunk):
            grid_side[c * chunk + b] = grid_enc[b * NODE_BLOCK : (b + 1) * NODE_BLOCK].T
    for copy in small[1:]:
        copy.wait()
    mesh_enc = dot3(mesh_rows[...], mesh_w_here[...])
    for b in range(node_blocks):
        mesh_side[b] = mesh_enc[b * NODE_BLOCK : (b + 1) * NODE_BLOCK].T

    def before(source, target, from_ids, to_ids):
        return picked(grid_side[source], from_ids) + picked(mesh_side[target], to_ids)

    add_messages(listed, taken, edges_here, before, messages, sums)
    for b in range(node_blocks):
        out[b * NODE_BLOCK : (b + 1) * NODE_BLOCK, :] = sums[b].T


def halves(got, other, rows):
    mine, theirs = got[rows, :], other[rows, :]
    first = lax.axis_index("nodes") % 2 == 0
    return jnp.concatenate(
        [jnp.where(first, mine, theirs), jnp.where(first, theirs, mine)], axis=0
    )


def spread(lefts, own_w, got, other, rows):
    depth, width = own_w.shape
    added = [0.0] * (width // NODE_BLOCK)
    for step, left in enumerate(lefts):
        left = parts(left)
        weight = own_w[...] if step == 0 else halves(got[step - 1], other[step - 1], rows)
        for j in range(width // NODE_BLOCK):
            if step == 0:
                block = weight[:, j * NODE_BLOCK : (j + 1) * NODE_BLOCK]
            else:
                block = weight[j * depth : (j + 1) * depth]
            added[j] = added[j] + dot3(left, block)
    return jnp.concatenate(added, axis=1)


def pack_kernel(count, out_w, dec_mesh_w, dec_grid_w, dec_out_w, *refs):
    half = lax.axis_index("nodes") % 2
    me = lax.axis_index("mp")
    share = dec_out_w.shape[1] // count
    blocks = [
        out_w[:, j * NODE_BLOCK : (j + 1) * NODE_BLOCK]
        for j in range(out_w.shape[1] // NODE_BLOCK)
    ]
    lower = len(blocks) // 2
    chosen = jnp.where(
        half == 0, jnp.concatenate(blocks[:lower], axis=0), jnp.concatenate(blocks[lower:], axis=0)
    )
    rows = dec_mesh_w.shape[0] // 2
    mine = pl.ds(pl.multiple_of(half * rows, rows), rows)

    def columns_of(index):
        return dec_out_w[:, pl.ds(pl.multiple_of(index * share, share), share)]

    refs[0][...] = columns_of(me)
    for step in range(1, count):
        out = refs[step]
        top = chosen.shape[0]
        out[:top, :] = chosen
        out[top : top + rows, :] = dec_mesh_w[mine, :]
        out[top + rows : top + 2 * rows, :] = dec_grid_w[mine, :]
        out[top + 2 * rows :, :] = columns_of(partner(me, step, count))


def middle_kernel(count, *refs):
    mesh_latent, gain, query_w, key_w, value_w, own_w = refs[:6]
    sums = refs[6 : 6 + count]
    got_w = refs[6 + count : 5 + 2 * count]
    other_w = refs[5 + 2 * count : -4]
    mesh_one_ref, normed_ref, query_ref, key_value_ref = refs[-4:]
    lefts = [piece[...] for piece in sums]
    half = slice(0, own_w.shape[0] * own_w.shape[1] // NODE_BLOCK // 2)
    mesh_one = mesh_latent[...] + spread(lefts, own_w, got_w, other_w, half)
    normed = layer_norm(mesh_one, gain[...])
    mesh_one_ref[...] = mesh_one
    normed_ref[...] = normed
    query_ref[...] = dot_exact(normed, query_w[...])
    cols = key_w.shape[1]
    key_value_ref[:, :cols] = dot_exact(normed, key_w[...])
    key_value_ref[:, cols:] = dot3(normed, value_w[...])


def hidden_kernel(count, normed, up_w, down_w, *refs):
    out, scratch = refs[:-1], refs[-1]
    hidden = silu(dot3(normed[...], up_w[...]))
    scratch[...] = dot3(hidden, down_w[...])
    rows, cols = normed.shape[0] // count, out[0].shape[1]
    me = lax.axis_index("mp")
    for step in range(count):
        piece = scratch[pl.ds(partner(me, step, count) * rows, rows), :]
        for j in range(piece.shape[1] // cols):
            out[step][j * rows : (j + 1) * rows, :] = piece[:, j * cols : (j + 1) * cols]


def attention_kernel(count, heads, order, neighbor_blocks, query, hidden, *refs):
    pieces, received, (out, scores, named) = refs[:count], refs[count:-3], refs[-3:]
    me = lax.axis_index("nodes")
    hidden_sum = hidden[...]
    for other in received:
        hidden_sum = hidden_sum + other[...]
    out[query.shape[0] :, :] = hidden_sum
    blocks = query.shape[0] // NODE_BLOCK
    cols = query.shape[1]
    for q in range(blocks):

        def clear(i, carry):
            named[i] = 0
            return carry

        def count_in(i, carry):
            listed = neighbor_blocks[me * blocks + q, i]
            named[listed] = named[listed] + 1
            return carry

        lax.fori_loop(0, named.shape[0], clear, 0)
        lax.fori_loop(0, neighbor_blocks.shape[1], count_in, 0)
        for h in range(heads):
            lanes = slice(h * HEAD_DIM, (h + 1) * HEAD_DIM)
            own = query[q * NODE_BLOCK : (q + 1) * NODE_BLOCK, lanes] * (1.0 / math.sqrt(HEAD_DIM))
            top = jnp.full((NODE_BLOCK, 1), -1e30, F32)
            for i in range(count):
                for b in range(blocks):
                    keys = pieces[i][b * NODE_BLOCK : (b + 1) * NODE_BLOCK, lanes]
                    score = lax.dot_general(
                        own,
                        keys,
                        (((1,), (1,)), ((), ())),
                        precision=EXACT,
                        preferred_element_type=F32,
                    )
                    score = jnp.where(named[order(me)[i] * blocks + b] > 0, score, -1e30)
                    scores[i * blocks + b] = score
                    top = jnp.maximum(top, jnp.max(score, axis=-1, keepdims=True))
            total = jnp.zeros((NODE_BLOCK, 1), F32)
            result = jnp.zeros((NODE_BLOCK, HEAD_DIM), F32)
            value_lanes = slice(cols + h * HEAD_DIM, cols + (h + 1) * HEAD_DIM)
            for i in range(count):
                for b in range(blocks):
                    times = named[order(me)[i] * blocks + b].astype(F32)
                    weight = jnp.exp(scores[i * blocks + b] - top) * times
                    total = total + jnp.sum(weight, axis=-1, keepdims=True)
                    values = pieces[i][b * NODE_BLOCK : (b + 1) * NODE_BLOCK, value_lanes]
                    result = result + dot3(weight, values)
            out[q * NODE_BLOCK : (q + 1) * NODE_BLOCK, lanes] = result / total


def after_kernel(count, *refs):
    mesh_one, gain, own_out_w, own_mesh_w = refs[:4]
    attended = refs[4 : 4 + count]
    got = refs[4 + count : 3 + 2 * count]
    other = refs[3 + 2 * count : -2]
    out, total = refs[-2:]
    nodes, width = mesh_one.shape
    depth = attended[0].shape[1]
    half = own_out_w.shape[0] * own_out_w.shape[1] // NODE_BLOCK // 2
    tall = own_mesh_w.shape[0] // 2
    me = lax.axis_index("mp")
    lefts = [piece[:nodes] for piece in attended]
    total[...] = mesh_one[...] + spread(lefts, own_out_w, got, other, slice(0, half))
    rows = nodes // count
    for step in range(count):
        place = pl.ds(partner(me, step, count, back=True) * rows, rows)
        for j in range(width // depth):
            total[place, j * depth : (j + 1) * depth] += attended[step][
                nodes + j * rows : nodes + (j + 1) * rows
            ]
    normed = parts(layer_norm(total[...], gain[...]))
    for step in range(count):
        if step == 0:
            weight = own_mesh_w[...]
        else:
            weight = halves(got[step - 1], other[step - 1], slice(half, half + tall))
        projected = dot3(normed, weight)
        cols = weight.shape[1]
        out[step * cols : (step + 1) * cols, :] = projected.T


def grid_kernel(count, skip, *refs):
    grid_latent, own_w = refs[:2]
    got, other = refs[2 : 1 + count], refs[1 + count : -5]
    out, grid_rows, high, low, sems = refs[-5:]
    copies = row_chunks(grid_latent, grid_rows, sems)
    for copy in copies:
        copy.start()
    cols = own_w.shape[1]
    tall = own_w.shape[0] // 2
    for step in range(count):
        lanes = slice(step * cols, (step + 1) * cols)
        if step == 0:
            weight = own_w[...]
        else:
            weight = halves(got[step - 1], other[step - 1], slice(skip, skip + tall))
        high[:, lanes], low[:, lanes] = parts(weight)
    rows = grid_rows.shape[0] // len(copies)
    chunk = rows // NODE_BLOCK
    for c, copy in enumerate(copies):
        copy.wait()
        grid_dec = dot3(grid_rows[c * rows : (c + 1) * rows], (high[...], low[...]))
        for b in range(chunk):
            out[c * chunk + b] = grid_dec[b * NODE_BLOCK : (b + 1) * NODE_BLOCK].T


def decoder_kernel(count, node_blocks, all_blocks, own_tiles, *refs):
    tiles, edges, grid_side, base = refs[:4]
    weights = refs[4 : 4 + count]
    if own_tiles:
        sides = refs[4 + count : -7]
        out, mesh_side, messages, listed, sums, columns, sem = refs[-7:]
        share = columns.shape[1]
        first = pl.multiple_of(lax.axis_index("mp") * share, share)
        copy = pltpu.make_async_copy(base.at[:, pl.ds(first, share)], columns, sem)
        copy.start()
        base = columns
    else:
        sides = refs[4 + count : -5]
        out, mesh_side, messages, listed, sums = refs[-5:]
    grid_blocks = grid_side.shape[0]
    me = lax.axis_index("nodes")
    for i, side in enumerate(sides):
        for b in range(node_blocks):
            block = side[:, b * NODE_BLOCK : (b + 1) * NODE_BLOCK]
            mesh_side[i * node_blocks + b] = side_by_side(block)
    sums[...] = jnp.zeros_like(sums)

    def sort_in(t, taken):
        away = lax.rem(tiles[0, t] - (me - 1) * node_blocks + all_blocks, all_blocks)
        owner = away // node_blocks
        source = lax.rem(away, node_blocks)
        if own_tiles:
            takes = owner == 1
        else:
            takes = owner != 1
            source = source + jnp.where(owner == 0, 0, node_blocks)
        listed[0, taken] = t
        listed[1, taken] = source
        listed[2, taken] = tiles[1, t] - me * grid_blocks
        return taken + takes.astype(jnp.int32)

    taken = lax.fori_loop(0, edges.shape[0], sort_in, 0)
    fill(listed, taken, messages.shape[0], grid_blocks)

    def before(source, target, from_ids, to_ids):
        hot = one_hot(from_ids)
        from_mesh = mm(mesh_side[source], jnp.concatenate([hot, hot], axis=0))
        return from_mesh + picked(grid_side[target], to_ids)

    add_messages(listed, taken, edges, before, messages, sums)
    high, low = parts(jnp.concatenate([w[...] for w in weights], axis=0).T)
    both = jnp.concatenate([high, low], axis=0)
    if own_tiles:
        copy.wait()
    rows = high.shape[0]
    for c in range(grid_blocks):
        place = slice(c * NODE_BLOCK, (c + 1) * NODE_BLOCK)
        sum_high, sum_low = parts(sums[c])
        twice = mm(both, sum_high)
        result = twice[:rows] + (twice[rows:] + mm(high, sum_low))
        out[place, :] = base[place, :] + result.T


def decoder_pass(own_tiles, node_blocks, all_blocks, tiles, edges, grid_side, base, weights, sides):
    grid_blocks, hidden, _ = grid_side.shape
    result = (grid_blocks * NODE_BLOCK, weights[0].shape[1])
    scratch = [
        pltpu.VMEM((len(sides) * node_blocks, hidden, 2 * NODE_BLOCK), BF16),
        pltpu.VMEM((GROUP, hidden, 2 * NODE_BLOCK), BF16),
        pltpu.SMEM((3, edges.shape[0] + GROUP), jnp.int32),
        pltpu.VMEM((grid_blocks + 1, hidden, NODE_BLOCK), F32),
    ]
    if own_tiles:
        scratch += [pltpu.VMEM(result, F32), pltpu.SemaphoreType.DMA]
    return call(
        functools.partial(decoder_kernel, len(weights), node_blocks, all_blocks, own_tiles),
        shape(*result),
        7 if own_tiles else 10,
        in_specs=smem(1)
        + vmem(2)
        + (hbm(1) if own_tiles else vmem(1))
        + vmem(len(weights) + len(sides)),
        out_specs=vmem(1)[0],
        scratch_shapes=scratch,
        compiler_params=limit(24),
    )(tiles, edges, grid_side, base, *weights, *sides)


def stacked(weight):
    return jnp.concatenate(
        [weight[:, j : j + NODE_BLOCK] for j in range(0, weight.shape[1], NODE_BLOCK)], axis=0
    )


def per_device(
    grid_latent,
    mesh_latent,
    enc_grid_w,
    enc_mesh_w,
    enc_out_w,
    block_gain,
    query_w,
    key_w,
    value_w,
    out_w,
    up_w,
    down_w,
    dec_gain,
    dec_grid_w,
    dec_mesh_w,
    dec_out_w,
    neighbor_blocks,
    enc_tiles,
    enc_edges,
    dec_tiles,
    dec_edges,
):
    me_node = lax.axis_index("nodes")
    nodes = lax.axis_size("nodes")
    mp = lax.axis_size("mp")
    steps = range(1, mp)
    grid_rows, width = grid_latent.shape
    node_rows = mesh_latent.shape[0]
    grid_blocks = grid_rows // NODE_BLOCK
    node_blocks = node_rows // NODE_BLOCK
    hidden_cols = enc_grid_w.shape[1]
    head_cols = query_w.shape[1]
    heads = head_cols // HEAD_DIM
    parity = me_node % 2
    chunks = 8 if grid_blocks % 8 == 0 else 1

    def my_half(weight):
        rows = weight.shape[0] // 2
        return lax.dynamic_slice_in_dim(weight, parity * rows, rows, 0)

    enc_half = my_half(stacked(enc_out_w))
    enc_got = [exchange(enc_half, "mp", k) for k in steps]
    enc_other = [exchange(g, "nodes", 1) for g in enc_got]

    enc_agg = call(
        functools.partial(encoder_kernel, grid_blocks, node_blocks),
        shape(node_rows, hidden_cols),
        8,
        in_specs=smem(1) + hbm(5),
        out_specs=vmem(1)[0],
        scratch_shapes=[
            pltpu.VMEM(grid_latent.shape, F32),
            pltpu.VMEM(enc_grid_w.shape, F32),
            pltpu.VMEM(mesh_latent.shape, F32),
            pltpu.VMEM(enc_mesh_w.shape, F32),
            pltpu.VMEM(enc_edges.shape, jnp.int32),
            pltpu.VMEM((grid_blocks, hidden_cols, NODE_BLOCK), F32),
            pltpu.VMEM((node_blocks, hidden_cols, NODE_BLOCK), F32),
            pltpu.VMEM((node_blocks + 1, hidden_cols, NODE_BLOCK), F32),
            pltpu.VMEM((ENC_GROUP, hidden_cols, 2 * NODE_BLOCK), BF16),
            pltpu.SMEM((3, enc_edges.shape[0] + ENC_GROUP), jnp.int32),
            pltpu.SemaphoreType.DMA((4 + chunks,)),
        ],
        compiler_params=limit(24),
    )(enc_tiles.T, *map(in_hbm, (grid_latent, enc_grid_w, mesh_latent, enc_mesh_w, enc_edges)))
    aggs = [enc_agg] + [exchange(enc_agg, "mp", k) for k in steps]

    mesh_one, normed, queries, key_values = call(
        functools.partial(middle_kernel, mp),
        (
            shape(node_rows, width),
            shape(node_rows, width),
            shape(node_rows, head_cols),
            shape(node_rows, 2 * head_cols),
        ),
        3,
        in_specs=vmem(4 + 3 * mp),
        out_specs=vmem(4),
        compiler_params=limit(24),
    )(
        in_hbm(mesh_latent),
        block_gain.reshape(1, -1),
        *map(in_hbm, (query_w, key_w, value_w)),
        in_hbm(enc_out_w),
        *aggs,
        *enc_got,
        *enc_other,
    )

    def order(me):
        if nodes % 2:
            return [(me - s) % nodes for s in range(nodes)]
        half = range(nodes // 2)
        return [(me - 2 * s) % nodes for s in half] + [((me ^ 1) - 2 * s) % nodes for s in half]

    if nodes % 2 == 0:
        far = [key_values] + [shifted(key_values, "nodes", 2 * s) for s in range(1, nodes // 2)]
        near = [exchange(piece, "nodes", 1) for piece in far]
        pieces = far + near
    else:
        pieces = [key_values] + [shifted(key_values, "nodes", s) for s in range(1, nodes)]

    share = dec_out_w.shape[1] // mp
    weight_rows = (out_w.size // NODE_BLOCK + dec_mesh_w.shape[0] + dec_grid_w.shape[0]) // 2
    out_columns, *sent = call(
        functools.partial(pack_kernel, mp),
        [shape(dec_out_w.shape[0], share)]
        + [shape(weight_rows + dec_out_w.shape[0], NODE_BLOCK)] * (mp - 1),
        2,
        in_specs=vmem(4),
        out_specs=vmem(mp),
        compiler_params=limit(16),
    )(*map(in_hbm, (out_w, dec_mesh_w, dec_grid_w, dec_out_w)))
    got = [exchange(sent[k - 1], "mp", k) for k in steps]
    other = [exchange(g, "nodes", 1) for g in got]
    dec_out = [out_columns] + [g[weight_rows:] for g in got]

    hidden = call(
        functools.partial(hidden_kernel, mp),
        [shape(node_rows // mp * (width // head_cols), head_cols)] * mp,
        2,
        in_specs=vmem(3),
        out_specs=vmem(mp),
        scratch_shapes=[pltpu.VMEM((node_rows, width), F32)],
        compiler_params=limit(24),
    )(normed, in_hbm(up_w), in_hbm(down_w))
    hidden_got = [exchange(hidden[k], "mp", k) for k in steps]

    attended = call(
        functools.partial(attention_kernel, nodes, heads, order),
        shape(node_rows + hidden[0].shape[0], head_cols),
        3,
        in_specs=smem(1) + vmem(1 + mp + nodes),
        out_specs=vmem(1)[0],
        scratch_shapes=[
            pltpu.VMEM((nodes * node_blocks, NODE_BLOCK, NODE_BLOCK), F32),
            pltpu.SMEM((nodes * node_blocks,), jnp.int32),
        ],
        compiler_params=limit(24),
    )(neighbor_blocks, queries, hidden[0], *pieces, *hidden_got)
    attends = [attended] + [exchange(attended, "mp", k) for k in steps]

    dec_cols = dec_mesh_w.shape[1]
    mesh_dec = call(
        functools.partial(after_kernel, mp),
        shape(mp * dec_cols, node_rows),
        3,
        in_specs=vmem(2 + 3 * mp),
        out_specs=vmem(1)[0],
        scratch_shapes=[pltpu.VMEM((node_rows, width), F32)],
        compiler_params=limit(24),
    )(
        mesh_one,
        dec_gain.reshape(1, -1),
        out_w,
        dec_mesh_w,
        *attends,
        *got,
        *other,
    )

    skip = out_w.shape[0] * width // NODE_BLOCK // 2 + dec_mesh_w.shape[0] // 2
    grid_side = call(
        functools.partial(grid_kernel, mp, skip),
        shape(grid_blocks, mp * dec_cols, NODE_BLOCK),
        6,
        in_specs=hbm(1) + vmem(2 * mp - 1),
        out_specs=vmem(1)[0],
        scratch_shapes=[
            pltpu.VMEM(grid_latent.shape, F32),
            pltpu.VMEM((width, mp * dec_cols), BF16),
            pltpu.VMEM((width, mp * dec_cols), BF16),
            pltpu.SemaphoreType.DMA((chunks,)),
        ],
        compiler_params=limit(24),
    )(in_hbm(grid_latent), dec_grid_w, *got, *other)

    before = shifted(mesh_dec, "nodes", 1)
    behind = shifted(mesh_dec, "nodes", -1)
    decode = functools.partial(
        decoder_pass,
        node_blocks=node_blocks,
        all_blocks=node_blocks * nodes,
        tiles=dec_tiles.T,
        edges=dec_edges,
        grid_side=grid_side,
        weights=dec_out,
    )
    nearest = decode(True, base=in_hbm(grid_latent), sides=[mesh_dec])
    return decode(False, base=nearest, sides=[before, behind])


def solution(mesh):
    in_specs = (
        P("nodes", None),
        P("nodes", None),
        P(None, "mp"),
        P(None, "mp"),
        P("mp", None),
        P(),
        P(None, "mp"),
        P(None, "mp"),
        P(None, "mp"),
        P("mp", None),
        P(None, "mp"),
        P("mp", None),
        P(),
        P(None, "mp"),
        P(None, "mp"),
        P("mp", None),
        P(),
        P("nodes", None),
        P("nodes", None, None),
        P("nodes", None),
        P("nodes", None, None),
    )
    out_specs = P("nodes", "mp")

    return jax.shard_map(
        per_device, mesh=mesh, in_specs=in_specs, out_specs=out_specs, check_vma=False
    )
```
